512 devices in a mesh: grp: 32 (over y, x), mem: 16 (over z, core).
Axes of the slice: x: 4, y: 8, z: 8, core: 2. Of those that a mesh axis runs over, the one named last changes fastest.
Arguments:
- a_tiles: bfloat16 [16384, 128, 128], P(('grp', 'mem')), may hold values from -0.5 to 0.5
- b_tiles: bfloat16 [128, 128, 128], P('grp'), may hold values from -6 to 6
- mask_ref: int32 [16384, 24], P(('grp', 'mem')), may hold values from 0 to 31, as said below
- b_ref: int32 [16384, 24], P(('grp', 'mem')), may hold values from 0 to 127
- tile_strip: int32 [16384], P(('grp', 'mem')), may hold values from 0 to 31
- item_count: int32 [512], P(('grp', 'mem')), may hold values from 8 to 32
Outputs:
- strip_count: float32 [1024], P(('grp', 'mem'))
The draws below stay inside these ranges and needn't reach their ends.
Inputs may be any that keep to these rules, and one draw needn't show every extreme that they name: mask_ref[t, p] and t % 32 have the same remainder modulo the number of devices of axis mem.
All inputs are finite; a program needn't handle non-finite values.
Results may differ from the reference program's by a relative error of at most 0.0003.
Values may be sent and summed in bfloat16 or wider, within the bound.
A program may use at most 64 MiB of HBM per device.

```python
import math
import jax
import jax.numpy as jnp
import numpy as np
from jax import lax

TILE = 128
PARTNERS = 24
ITEM_DEV = 32
ITEMS = 16384
BTILES = 128
STRIP_GRP = 32
STRIPS = 1024
DEVS = 512
N_MEM = 16


def draw_mask_ref(key, part):
    position = jnp.arange(ITEMS, dtype=jnp.int32)
    residue = position % ITEM_DEV % N_MEM
    picks = jax.random.randint(key, (ITEMS, PARTNERS), 0, ITEM_DEV // N_MEM, dtype=jnp.int32)
    return (residue[:, None] + N_MEM * picks).astype(jnp.int32)


def plant(entries, key, low, top_value):
    longest = entries.shape.index(max(entries.shape))
    spots = []
    for shift in (0, 1):
        where = [jax.random.randint(jax.random.fold_in(key, axis), (), 0, length) for axis, length in enumerate(entries.shape)]
        where[longest] = (where[longest] + shift) % entries.shape[longest]
        spots.append(tuple(where))
    return entries.at[spots[0]].set(low).at[spots[1]].set(top_value)


def block_levels(stream_key, extent, cuts, low, top_value):
    gain, own = 1.0, jax.random.fold_in(stream_key, 6)
    for dim, blocks in cuts:
        heights = jnp.exp(jax.random.uniform(jax.random.fold_in(own, dim), (blocks,), jnp.float32, low / len(cuts), top_value / len(cuts)))
        gain = gain * jnp.repeat(heights, extent[dim] // blocks).reshape([-1 if axis == dim else 1 for axis in range(len(extent))])
    return gain


def rank_bounds(number_of, slope):
    weights = [(1 << 20) // math.isqrt(grade ** slope) + 1 for grade in range(1, number_of + 1)]
    spread = 1 + sum(weights) // (1 << 30)
    return np.cumsum(np.array([max(1, weight // spread) for weight in weights]))


def ranked(stream_key, shape, count, lean):
    grid = rank_bounds(count, lean)
    pick = jax.random.randint(jax.random.fold_in(stream_key, 1), shape, 0, int(grid[count - 1]))
    rank = jnp.searchsorted(jnp.asarray(grid, jnp.int32), pick, side="right")
    return jax.random.permutation(jax.random.fold_in(stream_key, 2), count)[rank].astype(jnp.int32)


def normal_values(key, extent, deviation, limit, split=(), held_as=jnp.bfloat16):
    factor_of = block_levels(key, extent, split, -0.22, 0.18) if split else 1.0
    array = jax.random.normal(key, extent, jnp.float32) * deviation * factor_of
    return jnp.minimum(jnp.maximum(array, -limit), limit).astype(held_as)


def setup_inputs(seed: int = 0) -> dict:
    streams_of = jax.random.split(jax.random.key(seed), 7)
    return {
        "a_tiles": normal_values(streams_of[0], (ITEMS, TILE, TILE), TILE ** -0.5, 0.5, ((0, 512),)),
        "b_tiles": normal_values(streams_of[1], (BTILES, TILE, TILE), 1.0, 6.0, ((0, 32),)),
        "mask_ref": draw_mask_ref(jax.random.fold_in(streams_of[6], 71), 0),
        "b_ref": plant(ranked(streams_of[3], (ITEMS, PARTNERS), BTILES, 2), jax.random.fold_in(streams_of[3], 3), 0, BTILES - 1).astype(jnp.int32),
        "tile_strip": plant(jax.random.randint(streams_of[4], (ITEMS,), 0, STRIP_GRP), jax.random.fold_in(streams_of[4], 1), 0, STRIP_GRP - 1).astype(jnp.int32),
        "item_count": plant(jax.random.randint(streams_of[5], (DEVS,), ITEM_DEV // 4, ITEM_DEV + 1), jax.random.fold_in(streams_of[5], 1), ITEM_DEV // 4, ITEM_DEV).astype(jnp.int32),
    }


def reference(a_tiles, b_tiles, mask_ref, b_ref, tile_strip, item_count):
    items = a_tiles.shape[0]
    index = jnp.arange(items, dtype=jnp.int32)
    owner = (index // ITEM_DEV).astype(jnp.int32)
    mask_index = (owner[:, None] * ITEM_DEV + mask_ref).astype(jnp.int32)
    live = ((index % ITEM_DEV) < item_count[owner]).astype(jnp.float32)

    def one_tile(args):
        tile_index, refs, closers = args
        left = a_tiles[tile_index].astype(jnp.float32)
        middle = b_tiles[refs].astype(jnp.float32)
        closing = a_tiles[closers].astype(jnp.float32)
        product = jnp.einsum("ij,pjk->pik", left, middle, precision=lax.Precision.HIGHEST)
        return jnp.sum(product * closing)

    values = lax.map(one_tile, (index, b_ref, mask_index), batch_size=16) * live
    strip = ((index // (ITEM_DEV * N_MEM)) * STRIP_GRP + tile_strip).astype(jnp.int32)
    return jax.ops.segment_sum(values, strip, num_segments=STRIPS)
```

```python
import jax
import jax.numpy as jnp
from jax import lax
from jax.experimental import pallas as pl
from jax.experimental.pallas import tpu as pltpu
from jax.sharding import PartitionSpec as P

NX, NY, NZ = 4, 8, 8
TILE = 128
ITEM_DEV = 32
PARTNERS = 24
HOPS = (0, 1, 7, 2, 6, 3, 5, 4)
MESH = pl.DeviceIdType.MESH
F32, BF16, I32 = jnp.float32, jnp.bfloat16, jnp.int32


def iota(shape, dim):
    return lax.broadcasted_iota(I32, shape, dim)


def kernel(a_hbm, b_hbm, mask_ref, bref_ref, strip_ref, count_ref, out_ref,
           a_buf, m_buf, n_buf, meta, g_buf, kw_buf, oh_buf, acc, p_buf, r_buf,
           loc_sem, y_s, y_r, x_s, x_r, f_s, f_r, z_s, z_r, c_s, c_r, e_s, e_r):
    grp = lax.axis_index("grp")
    mem = lax.axis_index("mem")
    gy, gx = grp // NX, grp % NX
    z, core = mem // 2, mem % 2
    u = z % 2
    zu = ((z + 1) % NZ) * 2 + core
    zd = ((z + NZ - 1) % NZ) * 2 + core
    xr = gy * NX + (gx + 1) % NX
    xl = gy * NX + (gx + NX - 1) % NX
    ydev = [((gy + HOPS[q]) % NY) * NX + gx for q in range(NY)]
    sib = z * 2 + (1 - core)

    own_m = pltpu.make_async_copy(b_hbm.at[2 * core + u], m_buf.at[0], loc_sem.at[0])
    own_n = pltpu.make_async_copy(b_hbm.at[2 * core + (1 - u)], n_buf.at[0], loc_sem.at[1])
    own_a = pltpu.make_async_copy(a_hbm, a_buf.at[pl.ds(0, ITEM_DEV)], loc_sem.at[2])
    own_m.start()
    own_a.start()
    own_n.start()

    barrier = pltpu.get_barrier_semaphore()
    for q in range(1, NY):
        pl.semaphore_signal(barrier, inc=1, device_id=(ydev[q], mem), device_id_type=MESH)
    for gg in (xl, xr):
        pl.semaphore_signal(barrier, inc=1, device_id=(gg, mem), device_id_type=MESH)
    for o in range(1, 16):
        pl.semaphore_signal(barrier, inc=1, device_id=(grp, (mem + o) % 16), device_id_type=MESH)

    meta[0] = jnp.full((32, 128), -1, I32)
    meta[0, 0:PARTNERS, 0:ITEM_DEV] = bref_ref[...] + 128 * (mask_ref[...] >> 4)
    lane = iota((1, ITEM_DEV), 1)
    meta[0, PARTNERS:PARTNERS + 1, 0:ITEM_DEV] = jnp.where(lane < count_ref[0], strip_ref[...], -1)
    acc[...] = jnp.zeros(acc.shape, F32)

    own_m.wait()
    pl.semaphore_wait(barrier, 24)

    def remote(src, dst, ss, rs, dev):
        return pltpu.make_async_remote_copy(
            src_ref=src, dst_ref=dst, send_sem=ss, recv_sem=rs, device_id=dev, device_id_type=MESH)

    def slot(q, dx):
        return q * 4 + dx

    ycopy = [None] + [
        remote(m_buf.at[0], m_buf.at[slot(q, 0)], y_s.at[q], y_r.at[q], (ydev[q], mem)) for q in range(1, NY)]
    xright = [remote(m_buf.at[slot(q, 0)], m_buf.at[slot(q, 1)], x_s.at[q], x_r.at[q], (xr, mem)) for q in range(NY)]
    xleft = [remote(m_buf.at[slot(q, 0)], m_buf.at[slot(q, 3)], x_s.at[8 + q], x_r.at[8 + q], (xl, mem)) for q in range(NY)]
    fwd = [remote(m_buf.at[slot(q, 1 if q % 2 == 0 else 3)], m_buf.at[slot(q, 2)], f_s.at[q], f_r.at[q],
                  (xr if q % 2 == 0 else xl, mem)) for q in range(NY)]
    zcopy = [None] + [
        remote(m_buf.at[s], n_buf.at[s], z_s.at[s], z_r.at[s], (grp, zu if (s // 4 + s) % 2 == 0 else zd))
        for s in range(1, 32)]
    metacopy = remote(meta.at[0], meta.at[1], c_s.at[0], c_r.at[0], (grp, sib))
    acopy = remote(a_buf.at[pl.ds(0, ITEM_DEV)], a_buf.at[pl.ds(ITEM_DEV, ITEM_DEV)], c_s.at[1], c_r.at[1], (grp, sib))

    xright[0].start()
    xleft[0].start()
    for q in range(1, NY):
        ycopy[q].start()
    metacopy.start()
    own_a.wait()
    acopy.start()

    def products(d):
        def body(i, carry):
            x = jnp.concatenate([a_buf[d * 32 + i], a_buf[d * 32 + 16 + i]], axis=1)
            c = lax.dot_general(x, x, (((0,), (0,)), ((), ())), preferred_element_type=F32)
            for ti in range(2):
                for k in range(2):
                    g_buf[k * 64 + d * 32 + ti * 16 + i] = c[ti * 128:(ti + 1) * 128, k * 128:(k + 1) * 128]
            return carry
        return body

    def got_y(q):
        ycopy[q].wait_recv()
        xright[q].start()
        xleft[q].start()
        zcopy[slot(q, 0)].start()

    def got_x(q):
        xright[q].wait_recv()
        xleft[q].wait_recv()
        fwd[q].start()
        zcopy[slot(q, 1)].start()
        zcopy[slot(q, 3)].start()

    def got_f(q):
        fwd[q].wait_recv()
        zcopy[slot(q, 2)].start()

    def build_weights():
        metacopy.wait_recv()
        codes = jnp.concatenate([meta[0, 0:PARTNERS, 0:32], meta[1, 0:PARTNERS, 0:32]], axis=1)
        r = iota((64, 1), 0)
        s = r % 32
        q, dx = s // 4, s % 4
        hop = jnp.zeros((64, 1), I32)
        for n in range(1, NY):
            hop = jnp.where(q == n, HOPS[n], hop)
        owner = ((gy + NY - hop) % NY) * NX + (gx + NX - dx) % NX
        tile = owner * 4 + 2 * core + jnp.where(r < 32, u, 1 - u)
        parts = []
        for k in range(2):
            w = jnp.zeros((64, 64), F32)
            for p in range(PARTNERS):
                w = w + (codes[p:p + 1, :] == tile + 128 * k).astype(F32)
            parts.append(w)
        w = jnp.concatenate(parts, axis=1).astype(BF16)
        spread = (iota((64, 1024), 0) == iota((64, 1024), 1) // 16).astype(BF16)
        wide = lax.dot_general(w, spread, (((0,), (0,)), ((), ())), preferred_element_type=F32)
        diag = (iota((256, 1024), 0) % 16 == iota((256, 1024), 1) % 16).astype(F32)
        for nb in range(8):
            rows = jnp.broadcast_to(wide[nb * 16:(nb + 1) * 16, None, :], (16, 16, 1024)).reshape(256, 1024)
            kw_buf[nb] = (rows * diag).astype(BF16)
        row = iota((128, 128), 0)
        target = jnp.where(row % 8 < 2, (row // 8) * 2 + row % 8, -2)
        oh = jnp.zeros((128, 1024), F32)
        for d in range(2):
            hot = (target == meta[d, PARTNERS:PARTNERS + 1, :]).astype(BF16)
            rep = ((iota((128, 1024), 1) // 8) % 64 - d * 32 == iota((128, 1024), 0)).astype(BF16)
            oh = oh + jnp.dot(hot, rep, preferred_element_type=F32)
        oh_buf[...] = oh.astype(BF16)

    def run_pass(buf, s0, rb):
        def body(nb, carry):
            lhs = kw_buf[nb, :, rb * 256:(rb + 1) * 256]
            n0 = pl.multiple_of(nb * 16, 16)
            total = acc[pl.ds(n0, 16)]
            for jp in range(4):
                j = jp * 32
                right = jnp.concatenate([buf[s0:s0 + 16, j:j + 16, :].reshape(256, 128),
                                         buf[s0:s0 + 16, j + 16:j + 32, :].reshape(256, 128)], axis=1)
                w = jnp.dot(lhs, right, preferred_element_type=F32)
                g0 = g_buf[pl.ds(n0, 16), j:j + 16, :]
                g1 = g_buf[pl.ds(n0, 16), j + 16:j + 32, :]
                prod = w[:, :128].reshape(16, 16, 128) * g0 + w[:, 128:].reshape(16, 16, 128) * g1
                total = total + (prod[:, :8] + prod[:, 8:])
            acc[pl.ds(n0, 16)] = total
            return carry
        lax.fori_loop(0, 8, body, 0)

    lax.fori_loop(0, 8, products(0), 0)
    got_x(0)
    got_y(1)
    got_y(2)
    lax.fori_loop(8, 16, products(0), 0)
    got_f(0)
    got_x(1)
    got_x(2)
    got_y(3)
    got_y(4)
    build_weights()
    got_f(1)
    got_f(2)
    got_x(3)
    got_x(4)
    got_y(5)
    got_y(6)
    acopy.wait_recv()
    lax.fori_loop(0, 8, products(1), 0)
    got_f(3)
    got_f(4)
    got_x(5)
    got_x(6)
    got_y(7)
    lax.fori_loop(8, 16, products(1), 0)
    got_f(5)
    got_f(6)
    got_x(7)
    run_pass(m_buf, 0, 0)
    got_f(7)
    run_pass(m_buf, 16, 1)
    own_n.wait()
    for s in range(1, 16):
        zcopy[s].wait_recv()
    run_pass(n_buf, 0, 2)
    for s in range(16, 32):
        zcopy[s].wait_recv()
    run_pass(n_buf, 16, 3)

    rest = acc[...].reshape(1024, 128)
    sums = jnp.zeros((128, 128), F32)
    for _ in range(3):
        part = rest.astype(BF16)
        rest = rest - part.astype(F32)
        sums = sums + jnp.dot(oh_buf[...], part, preferred_element_type=F32)
    p_buf[...] = sums.reshape(16, 8, 128)

    ends = [None] + [
        remote(p_buf.at[(mem + o) % 16], r_buf.at[o], e_s.at[o], e_r.at[o], (grp, (mem + o) % 16))
        for o in range(1, 16)]
    for o in range(1, 16):
        ends[o].start()
    total = p_buf[mem]
    for o in range(1, 16):
        ends[o].wait_recv()
        total = total + r_buf[o]
    out_ref[0] = jnp.sum(total[0:1, :])
    out_ref[1] = jnp.sum(total[1:2, :])

    for copy in ycopy[1:] + xright + xleft + fwd + zcopy[1:] + [metacopy, acopy] + ends[1:]:
        copy.wait_send()


def shards(a_tiles, b_tiles, mask_ref, b_ref, tile_strip, item_count):
    dma = pltpu.SemaphoreType.DMA
    return pl.pallas_call(
        kernel,
        out_shape=jax.ShapeDtypeStruct((2,), F32),
        in_specs=[
            pl.BlockSpec(memory_space=pl.ANY),
            pl.BlockSpec(memory_space=pl.ANY),
            pl.BlockSpec(memory_space=pltpu.VMEM),
            pl.BlockSpec(memory_space=pltpu.VMEM),
            pl.BlockSpec(memory_space=pltpu.VMEM),
            pl.BlockSpec(memory_space=pltpu.SMEM),
        ],
        out_specs=pl.BlockSpec(memory_space=pltpu.SMEM),
        scratch_shapes=[
            pltpu.VMEM((64, TILE, TILE), BF16),
            pltpu.VMEM((32, TILE, TILE), BF16),
            pltpu.VMEM((32, TILE, TILE), BF16),
            pltpu.VMEM((2, 32, 128), I32),
            pltpu.VMEM((128, TILE, TILE), F32),
            pltpu.VMEM((8, 256, 1024), BF16),
            pltpu.VMEM((128, 1024), BF16),
            pltpu.VMEM((128, 8, 128), F32),
            pltpu.VMEM((16, 8, 128), F32),
            pltpu.VMEM((16, 8, 128), F32),
            dma((3,)),
            dma((8,)), dma((8,)),
            dma((16,)), dma((16,)),
            dma((8,)), dma((8,)),
            dma((32,)), dma((32,)),
            dma((2,)), dma((2,)),
            dma((16,)), dma((16,)),
        ],
        compiler_params=pltpu.CompilerParams(
            collective_id=0, has_side_effects=True, vmem_limit_bytes=56 * 1024 * 1024),
    )(a_tiles, b_tiles, mask_ref.T, b_ref.T, tile_strip.reshape(1, ITEM_DEV), item_count)


def solution(mesh):
    both = ("grp", "mem")
    in_specs = (P(both, None, None), P("grp", None, None), P(both, None), P(both, None), P(both), P(both))
    return jax.shard_map(shards, mesh=mesh, in_specs=in_specs, out_specs=P(both), check_vma=False)
```
